32 devices in a mesh: seq: 16 (over z, y, x), head: 2 (over core).
Axes of the slice: x: 2, y: 2, z: 4, core: 2. Of those that a mesh axis runs over, the one named last changes fastest.
Arguments:
- tokens: bfloat16 [8192, 3584], P('seq', 'head'), may hold values from -6 to 6
- pre_gain: float32 [3584], replicated, may hold values from 0.5 to 1.5
- query_weight: bfloat16 [3584, 2048], P(None, 'head'), may hold values from -0.375 to 0.375
- key_weight: bfloat16 [3584, 1024], P(None, 'head'), may hold values from -0.375 to 0.375
- value_weight: bfloat16 [3584, 1024], P(None, 'head'), may hold values from -0.09375 to 0.09375
- out_weight: bfloat16 [2048, 3584], P('head'), may hold values from -0.5 to 0.5
- post_gain: float32 [3584], P('head'), may hold values from 0.5 to 1.5
Outputs:
- layer_out: bfloat16 [8192, 3584], P('seq', 'head')
The draws below stay inside these ranges and needn't reach their ends.
All inputs are finite; a program needn't handle non-finite values.
Results may differ from the reference program's by a relative error of at most 0.013.
The reference program's roundings to bfloat16 on the way count: a program that leaves them out, or rounds other values in their place, can miss the bound.
Values may be sent and summed in bfloat16 or wider, within the bound.
A program may use at most 192 MiB of HBM per device.

```python
import jax
import jax.numpy as jnp
from jax import lax

D = 3584
QH = 8
KVH = 4
HD = 256
WINDOW = 4096
TOK_DEV = 512
TOKENS = 8192


def draw_out_weight(key, part):
    key_entries = jax.random.fold_in(key, 11)
    key_columns = jax.random.fold_in(key, 12)
    fan_in = QH * HD
    ramp = 3.0 ** (jnp.arange(D, dtype=jnp.float32) / D)
    column_scale = jnp.exp(jax.random.uniform(key_columns, (D,), jnp.float32) * jnp.log(10.0)) * ramp / 6.0
    entries = jax.random.truncated_normal(key_entries, -4.0, 4.0, (fan_in, D), jnp.float32)
    matrix = entries * column_scale[None, :] * (fan_in * 1.0) ** (-0.5)
    return jnp.clip(matrix, -0.5, 0.5).astype(jnp.bfloat16)


def block_scale(stream_key, shape, split, smallest, high):
    level = 1.0
    for dim, shards_of in split:
        steps = jax.random.uniform(jax.random.fold_in(jax.random.fold_in(stream_key, 6), dim), (shards_of,), jnp.float32, smallest / len(split), high / len(split))
        level = level * jnp.repeat(jnp.exp(steps), shape[dim] // shards_of).reshape((-1,) + (1,) * (len(shape) - 1 - dim))
    return level


def scatter_about(rng, shape, width, limit, pieces=(), held_as=jnp.bfloat16):
    drawn = width * jax.random.normal(rng, shape, jnp.float32)
    if pieces:
        drawn = drawn * block_scale(rng, shape, pieces, -0.22, 0.18)
    return jnp.clip(drawn, -limit, limit).astype(held_as)


def setup_inputs(seed: int = 0) -> dict:
    streams_of = jax.random.split(jax.random.key(seed), 8)
    return {
        "tokens": scatter_about(streams_of[0], (TOKENS, D), 1.0, 6.0, ((0, 16), (1, 2))),
        "pre_gain": jnp.clip(1.0 + 0.1 * jax.random.normal(streams_of[1], (D,), jnp.float32), 0.5, 1.5),
        "query_weight": scatter_about(streams_of[2], (D, QH * HD), (D // 16) ** -0.5, 0.375, ((1, 2),)),
        "key_weight": scatter_about(streams_of[3], (D, KVH * HD), (D // 16) ** -0.5, 0.375, ((1, 2),)),
        "value_weight": scatter_about(streams_of[4], (D, KVH * HD), D ** -0.5, 0.09375, ((1, 2),)),
        "out_weight": draw_out_weight(jax.random.fold_in(streams_of[7], 71), 0),
        "post_gain": jnp.clip(1.0 + 0.1 * jax.random.normal(streams_of[6], (D,), jnp.float32), 0.5, 1.5),
    }


softcap_limit = 50.0
rope_base = 10000.0
norm_epsilon = 1e-06

def rms_scale(values):
    return lax.rsqrt(lax.optimization_barrier(jnp.sum(values * values, axis=-1, keepdims=True)) / values.shape[-1] + norm_epsilon)

def rotate(values, positions):
    midpoint = values.shape[-1] // 2
    frequency = jnp.exp(-jnp.log(rope_base) * (2.0 * jnp.arange(midpoint, dtype=jnp.float32) / values.shape[-1]))
    angles = positions.astype(jnp.float32)[:, None] * frequency[None, :]
    cosine = jnp.cos(angles)[:, None, :]
    sine_part = jnp.sin(angles)[:, None, :]
    leading = values[..., :midpoint]
    trailing = values[..., midpoint:]
    return jnp.concatenate([leading * cosine - trailing * sine_part, trailing * cosine + leading * sine_part], axis=-1)

def reference(tokens, pre_gain, query_weight, key_weight, value_weight, out_weight, post_gain):
    widened = tokens.astype(jnp.float32)
    normed = (widened * rms_scale(widened) * pre_gain).astype(jnp.bfloat16)
    positions = jnp.arange(TOKENS, dtype=jnp.int32)
    queries = rotate(jnp.dot(normed, query_weight, preferred_element_type=jnp.float32).reshape(TOKENS, QH, HD), positions).astype(jnp.bfloat16)
    keys_all = rotate(jnp.dot(normed, key_weight, preferred_element_type=jnp.float32).reshape(TOKENS, KVH, HD), positions).astype(jnp.bfloat16)
    values_all = jnp.dot(normed, value_weight, preferred_element_type=jnp.float32).reshape(TOKENS, KVH, HD).astype(jnp.bfloat16)
    queries = lax.optimization_barrier(queries).astype(jnp.float32)
    keys_all = lax.optimization_barrier(keys_all).astype(jnp.float32)
    values_all = lax.optimization_barrier(values_all).astype(jnp.float32)
    group_size = QH // KVH
    padding = jnp.zeros((WINDOW, KVH, HD), jnp.float32)
    keys_padded = jnp.concatenate([padding, keys_all], axis=0)
    values_padded = jnp.concatenate([padding, values_all], axis=0)

    def one_block(block_index):
        first_row = block_index * TOK_DEV
        query_block = lax.dynamic_slice_in_dim(queries, first_row, TOK_DEV, 0).reshape(TOK_DEV, KVH, group_size, HD)
        key_block = lax.dynamic_slice_in_dim(keys_padded, first_row, WINDOW + TOK_DEV, 0)
        value_block = lax.dynamic_slice_in_dim(values_padded, first_row, WINDOW + TOK_DEV, 0)
        query_index = first_row + jnp.arange(TOK_DEV, dtype=jnp.int32)
        key_index = first_row - WINDOW + jnp.arange(WINDOW + TOK_DEV, dtype=jnp.int32)
        scores = jnp.einsum('qkgd,skd->kgqs', query_block, key_block) * HD ** (-0.5)
        capped = softcap_limit * jnp.tanh(scores / softcap_limit)
        offset = query_index[:, None] - key_index[None, :]
        allowed = (offset >= 0) & (offset < WINDOW) & (key_index[None, :] >= 0)
        weights = jnp.where(allowed, jnp.exp(capped), 0.0)
        denominator = lax.optimization_barrier(jnp.sum(weights, axis=-1))
        rounded = lax.optimization_barrier(weights.astype(jnp.bfloat16)).astype(jnp.float32)
        numerator = jnp.einsum('kgqs,skd->qkgd', rounded, value_block)
        attended_block = numerator / jnp.transpose(denominator, (2, 0, 1))[..., None]
        return attended_block.astype(jnp.bfloat16).reshape(TOK_DEV, QH * HD)
    attended = lax.map(one_block, jnp.arange(TOKENS // TOK_DEV, dtype=jnp.int32)).reshape(TOKENS, QH * HD)
    branch = jnp.dot(attended, out_weight, preferred_element_type=jnp.float32)
    return (widened + post_gain * branch * rms_scale(branch)).astype(jnp.bfloat16)
```

```python
import functools
import math

import jax
import jax.numpy as jnp
from jax import lax
from jax.experimental import pallas as pl
from jax.experimental.pallas import tpu as pltpu
from jax.sharding import PartitionSpec as P

HD = 256
WINDOW = 4096

softcap_limit = 50.0
rope_base = 10000.0
norm_epsilon = 1e-06

ROW_TILE = 256

X_KV, X_Q, Z_NEAR, Z_FAR, Y_NEAR, Y_FAR, X_OUT, MESSAGES = 0, 1, 2, 4, 6, 8, 10, 11


def attention_kernel(
    blocks, rows, q_ref, kv_ref, out_ref,
    held, queries, total, mass, leaving, landed, send_sems, recv_sems,
):
    group = 2 * 2
    me = lax.axis_index("seq")
    x = me % 2
    y = (me // 2) % 2
    x_mate = me + 1 - 2 * x
    y_mate = me + 2 - 4 * y
    z_next = me + group
    has_next = z_next < blocks
    has_prev = me >= group

    def copy(message, src, dst, device):
        return pltpu.make_async_remote_copy(
            src_ref=src,
            dst_ref=dst,
            send_sem=send_sems.at[message],
            recv_sem=recv_sems.at[message],
            device_id={"seq": device},
            device_id_type=pl.DeviceIdType.MESH,
        )

    barrier = pltpu.get_barrier_semaphore()

    def greet(device):
        pl.semaphore_signal(
            barrier, inc=1, device_id={"seq": device}, device_id_type=pl.DeviceIdType.MESH
        )

    greet(x_mate)
    greet(y_mate)
    pl.when(has_next)(lambda: greet(z_next))
    pl.when(has_prev)(lambda: greet(me - group))
    pl.semaphore_wait(barrier, 2 + has_next.astype(jnp.int32) + has_prev.astype(jnp.int32))

    own_kv = kv_ref.at[x]
    send_kv = copy(X_KV, kv_ref.at[1 - x], held.at[0, 1], x_mate)
    send_q = copy(X_Q, q_ref.at[1 - x], queries.at[1], x_mate)
    near = lambda r: own_kv if r == 0 else held.at[0, 1]
    z_near = [copy(Z_NEAR + r, near(r), held.at[2, r], z_next) for r in range(2)]
    z_far = [copy(Z_FAR + r, held.at[2, r], held.at[4, r], z_next) for r in range(2)]
    y_up_near = [copy(Y_NEAR + r, near(r), held.at[1, r], y_mate) for r in range(2)]
    y_up_far = [copy(Y_FAR + r, held.at[2, r], held.at[3, r], y_mate) for r in range(2)]
    y_down_near = [copy(Y_NEAR + r, held.at[2, r], held.at[1, r], y_mate) for r in range(2)]
    y_down_far = [copy(Y_FAR + r, held.at[4, r], held.at[3, r], y_mate) for r in range(2)]

    first_row = y == 0
    second_row = y == 1

    send_kv.start()
    pl.when(has_next)(lambda: z_near[0].start())
    pl.when(first_row)(lambda: y_up_near[0].start())
    send_q.start()

    queries[0] = q_ref[x]
    total[...] = jnp.zeros_like(total)
    mass[...] = jnp.zeros_like(mass)

    tiles_per_side = 2 * rows // ROW_TILE
    tiles_per_head = rows // ROW_TILE
    inner = 1.0 / (math.sqrt(HD) * softcap_limit)
    outer = softcap_limit / math.log(2.0)

    def attend(block, first, last, distances):
        def tile(t, carry):
            side = t // tiles_per_side
            within = t % tiles_per_side
            head = within // tiles_per_head
            start = pl.multiple_of((within % tiles_per_head) * ROW_TILE, ROW_TILE)
            q = queries[side, head, pl.ds(start, ROW_TILE), :]
            scores = lax.dot_general(
                q, block[0], (((1,), (1,)), ((), ())), preferred_element_type=jnp.float32
            )
            weights = jnp.exp2(outer * jnp.tanh(scores * inner))
            if distances is not None:
                distance = jnp.where(side == 0, distances[0], distances[1])
                offset = (
                    distance * rows
                    + start
                    + lax.broadcasted_iota(jnp.int32, weights.shape, 0)
                    - lax.broadcasted_iota(jnp.int32, weights.shape, 1)
                )
                weights = jnp.where((offset >= 0) & (offset < WINDOW), weights, 0.0)
            part = weights[:, :128]
            for k in range(1, rows // 128):
                part = part + weights[:, k * 128 : (k + 1) * 128]
            mass[side, head, pl.ds(start, ROW_TILE), :] += part
            total[side, head, pl.ds(start, ROW_TILE), :] += jnp.dot(
                weights.astype(jnp.bfloat16), block[1], preferred_element_type=jnp.float32
            )
            return carry

        lax.fori_loop(first, last, tile, 0)

    both = 2 * tiles_per_side
    def ahead(d, r, side):
        if side == r:
            return jnp.int32(2 * d)
        return 2 * d + (2 * x - 1 if side == 0 else 1 - 2 * x)

    def edge(d, r):
        return (ahead(d, r, 0), ahead(d, r, 1))

    reach = WINDOW // rows

    def bounds(d, r):
        low, high = edge(d, r)
        fits = lambda e: (e >= 0) & (e <= reach)
        first = jnp.where(fits(low), 0, tiles_per_side)
        last = jnp.where(fits(high), both, tiles_per_side)
        return first, last

    attend(own_kv, 0, tiles_per_side, edge(0, 0))

    send_kv.wait_recv()
    pl.when(has_next)(lambda: z_near[1].start())
    pl.when(first_row)(lambda: y_up_near[1].start())

    def forward_near(r):
        z_near[r].wait_recv()
        pl.when(has_next)(lambda: z_far[r].start())
        pl.when(first_row)(lambda: y_up_far[r].start())
        pl.when(second_row)(lambda: y_down_near[r].start())

    pl.when(has_prev)(lambda: forward_near(0))

    send_q.wait_recv()
    first, last = bounds(0, 0)
    attend(own_kv, tiles_per_side, last, edge(0, 0))
    first, last = bounds(0, 1)
    attend(held.at[0, 1], first, last, edge(0, 1))

    has_far = me >= 2 * group

    @pl.when(has_prev)
    def _():
        attend(held.at[2, 0], 0, both, None)

    @pl.when(me >= 2)
    def _():
        y_up_near[0].wait_recv()
        attend(held.at[1, 0], 0, both, None)

    @pl.when(has_prev)
    def _():
        forward_near(1)
        attend(held.at[2, 1], 0, both, None)

    def far(r):
        z_far[r].wait_recv()
        pl.when(second_row)(lambda: y_down_far[r].start())
        first, last = bounds(4, r)
        attend(held.at[4, r], first, last, edge(4, r))

    pl.when(has_far)(lambda: far(0))

    @pl.when(me >= 2)
    def _():
        y_up_near[1].wait_recv()
        attend(held.at[1, 1], 0, both, None)

    @pl.when(me >= 6)
    def _():
        y_up_far[0].wait_recv()
        attend(held.at[3, 0], 0, both, None)

    pl.when(has_far)(lambda: far(1))

    @pl.when(me >= 6)
    def _():
        y_up_far[1].wait_recv()
        attend(held.at[3, 1], 0, both, None)

    def finished(side, head):
        weight = jnp.sum(mass[side, head], axis=-1, keepdims=True)
        return (total[side, head] / weight).astype(jnp.bfloat16)

    for head in range(2):
        leaving[head] = finished(1, head)
    send_out = copy(X_OUT, leaving, landed, x_mate)
    for head in range(2):
        at = pl.multiple_of((2 * x + head) * HD, HD)
        value = finished(0, head)
        out_ref[:, pl.ds(at, HD)] = value
        if head == 0:
            send_out.start()
    send_out.wait_recv()
    for head in range(2):
        at = pl.multiple_of((2 * (1 - x) + head) * HD, HD)
        out_ref[:, pl.ds(at, HD)] = landed[head]

    send_kv.wait_send()
    send_q.wait_send()
    send_out.wait_send()
    for r in range(2):
        pl.when(has_next)(lambda: z_near[r].wait_send())
        pl.when(has_next & has_prev)(lambda: z_far[r].wait_send())
        pl.when(first_row)(lambda: y_up_near[r].wait_send())
        pl.when(first_row & has_prev)(lambda: y_up_far[r].wait_send())
        pl.when(second_row & has_prev)(lambda: y_down_near[r].wait_send())
        pl.when(second_row & has_far)(lambda: y_down_far[r].wait_send())


def attention(q, kv, blocks):
    rows = q.shape[2]
    half = (2, rows, HD)
    vmem = pl.BlockSpec(memory_space=pltpu.VMEM)
    return pl.pallas_call(
        functools.partial(attention_kernel, blocks, rows),
        out_shape=jax.ShapeDtypeStruct((rows, 4 * HD), jnp.bfloat16),
        in_specs=[vmem, vmem],
        out_specs=vmem,
        scratch_shapes=[
            pltpu.VMEM((5, 2) + half, jnp.bfloat16),
            pltpu.VMEM((2,) + half, jnp.bfloat16),
            pltpu.VMEM((2,) + half, jnp.float32),
            pltpu.VMEM((2, 2, rows, 128), jnp.float32),
            pltpu.VMEM(half, jnp.bfloat16),
            pltpu.VMEM(half, jnp.bfloat16),
            pltpu.SemaphoreType.DMA((MESSAGES,)),
            pltpu.SemaphoreType.DMA((MESSAGES,)),
        ],
        compiler_params=pltpu.CompilerParams(
            collective_id=0, has_side_effects=True, vmem_limit_bytes=48 * 1024 * 1024
        ),
    )(q, kv)


def swap_heads(shard):
    return lax.ppermute(shard, "head", [(0, 1), (1, 0)])


def rope_tables(positions):
    midpoint = HD // 2
    frequency = jnp.exp(
        -jnp.log(rope_base) * (2.0 * jnp.arange(midpoint, dtype=jnp.float32) / HD)
    )
    angles = positions.astype(jnp.float32)[:, None] * frequency[None, :]
    return jnp.cos(angles), jnp.sin(angles)


def rotated(head, cosine, sine):
    midpoint = HD // 2
    leading, trailing = head[:, :midpoint], head[:, midpoint:]
    return jnp.concatenate(
        [leading * cosine - trailing * sine, trailing * cosine + leading * sine], axis=-1
    ).astype(jnp.bfloat16)


def local(blocks, tokens, pre_gain, query_weight, key_weight, value_weight, out_weight, post_gain):
    rows, width = tokens.shape
    side = lax.axis_index("head")
    other = swap_heads(tokens)
    full = jnp.where(
        side == 0,
        jnp.concatenate([tokens, other], axis=1),
        jnp.concatenate([other, tokens], axis=1),
    )
    widened = full.astype(jnp.float32)
    scale = lax.rsqrt(
        jnp.sum(widened * widened, axis=-1, keepdims=True) / widened.shape[-1] + norm_epsilon
    )
    normed = (widened * scale * pre_gain).astype(jnp.bfloat16)
    positions = lax.axis_index("seq") * rows + jnp.arange(rows, dtype=jnp.int32)
    cosine, sine = rope_tables(positions)
    project = lambda weight: jnp.dot(normed, weight, preferred_element_type=jnp.float32)
    q_all, k_all, v_all = project(query_weight), project(key_weight), project(value_weight)
    head_of = lambda a, h: a[:, h * HD : (h + 1) * HD]
    q = jnp.stack(
        [
            jnp.stack([rotated(head_of(q_all, 2 * k + g), cosine, sine) for g in range(2)])
            for k in range(2)
        ]
    )
    kv = jnp.stack(
        [
            jnp.stack(
                [rotated(head_of(k_all, k), cosine, sine), head_of(v_all, k).astype(jnp.bfloat16)]
            )
            for k in range(2)
        ]
    )
    attended = attention(q, kv, blocks)
    mine = lax.dynamic_slice_in_dim(out_weight, side * width, width, 1)
    theirs = lax.dynamic_slice_in_dim(out_weight, (1 - side) * width, width, 1)
    given = jnp.dot(attended, theirs, preferred_element_type=jnp.float32).astype(jnp.bfloat16)
    arrived = swap_heads(given)
    kept = jnp.dot(attended, mine, preferred_element_type=jnp.float32)
    share = kept + arrived.astype(jnp.float32)
    squares = jnp.sum(share * share, axis=1, keepdims=True)
    squares = squares + swap_heads(squares)
    inverse_rms = lax.rsqrt(squares / (2 * width) + norm_epsilon)
    return (tokens.astype(jnp.float32) + post_gain * share * inverse_rms).astype(jnp.bfloat16)


def solution(mesh):
    placed = (
        P("seq", "head"),
        P(),
        P(None, "head"),
        P(None, "head"),
        P(None, "head"),
        P("head", None),
        P("head"),
    )
    return jax.shard_map(
        functools.partial(local, mesh.shape["seq"]),
        mesh=mesh,
        in_specs=placed,
        out_specs=P("seq", "head"),
        check_vma=False,
    )
```

```python
import functools
import math

import jax
import jax.numpy as jnp
from jax import lax
from jax.experimental import pallas as pl
from jax.experimental.pallas import tpu as pltpu
from jax.sharding import PartitionSpec as P

HD = 256
WINDOW = 4096

softcap_limit = 50.0
rope_base = 10000.0
norm_epsilon = 1e-06

ROW_TILE = 256

PIECES = 2
X_KV, X_Q, X_OUT, Z_NEAR, Z_FAR, Y_NEAR, Y_FAR, MESSAGES = 0, 2, 3, 5, 9, 13, 17, 21


def attention_kernel(
    blocks, rows, normed_ref, weight_ref, cosine_ref, sine_ref, kv_ref, out_ref,
    held, queries, asked, total, mass, leaving, landed, send_sems, recv_sems,
):
    group = 2 * 2
    me = lax.axis_index("seq")
    x = me % 2
    y = (me // 2) % 2
    x_mate = me + 1 - 2 * x
    y_mate = me + 2 - 4 * y
    z_next = me + group
    has_next = z_next < blocks
    has_prev = me >= group
    has_far = me >= 2 * group
    first_row = y == 0
    second_row = y == 1

    def copy(message, src, dst, device):
        return pltpu.make_async_remote_copy(
            src_ref=src,
            dst_ref=dst,
            send_sem=send_sems.at[message],
            recv_sem=recv_sems.at[message],
            device_id={"seq": device},
            device_id_type=pl.DeviceIdType.MESH,
        )

    barrier = pltpu.get_barrier_semaphore()

    def greet(device):
        pl.semaphore_signal(
            barrier, inc=1, device_id={"seq": device}, device_id_type=pl.DeviceIdType.MESH
        )

    greet(x_mate)
    greet(y_mate)
    pl.when(has_next)(lambda: greet(z_next))
    pl.when(has_prev)(lambda: greet(me - group))
    pl.semaphore_wait(barrier, 2 + has_next.astype(jnp.int32) + has_prev.astype(jnp.int32))

    pieces = [(r, h) for r in range(2) for h in range(PIECES)]
    near = lambda r, h: kv_ref.at[x, h] if r == 0 else held.at[0, 1, h]

    def copies(base, source, slot, device):
        return {
            (r, h): copy(base + PIECES * r + h, source(r, h), held.at[slot, r, h], device)
            for r, h in pieces
        }

    arrived = lambda slot: lambda r, h: held.at[slot, r, h]
    send_kv = [
        copy(X_KV + h, kv_ref.at[1 - x, h], held.at[0, 1, h], x_mate) for h in range(PIECES)
    ]
    send_q = copy(X_Q, asked, queries.at[1], x_mate)
    z_near = copies(Z_NEAR, near, 2, z_next)
    z_far = copies(Z_FAR, arrived(2), 4, z_next)
    y_up_near = copies(Y_NEAR, near, 1, y_mate)
    y_up_far = copies(Y_FAR, arrived(2), 3, y_mate)
    y_down_near = copies(Y_NEAR, arrived(2), 1, y_mate)
    y_down_far = copies(Y_FAR, arrived(4), 3, y_mate)

    for h in range(PIECES):
        send_kv[h].start()
        pl.when(has_next)(lambda: z_near[0, h].start())
        pl.when(first_row)(lambda: y_up_near[0, h].start())

    tiles_per_side = 2 * rows // ROW_TILE
    tiles_per_head = rows // ROW_TILE

    def ask(whose, store):
        def tile(t, carry):
            head = t // tiles_per_head
            start = pl.multiple_of((t % tiles_per_head) * ROW_TILE, ROW_TILE)
            at = pl.multiple_of((2 * whose + head) * HD, HD)
            value = jnp.dot(
                normed_ref[pl.ds(start, ROW_TILE), :],
                weight_ref[:, pl.ds(at, HD)],
                preferred_element_type=jnp.float32,
            )
            store(
                head,
                pl.ds(start, ROW_TILE),
                rotated(
                    value,
                    cosine_ref[pl.ds(start, ROW_TILE), :],
                    sine_ref[pl.ds(start, ROW_TILE), :],
                ),
            )
            return carry

        lax.fori_loop(0, tiles_per_side, tile, 0)

    def store_asked(head, where, value):
        asked[head, where, :] = value

    def store_own(head, where, value):
        queries[0, head, where, :] = value

    ask(1 - x, store_asked)

    def pass_mate(h):
        send_kv[h].wait_recv()
        pl.when(has_next)(lambda: z_near[1, h].start())
        pl.when(first_row)(lambda: y_up_near[1, h].start())

    def pass_near(r, h):
        z_near[r, h].wait_recv()
        pl.when(has_next)(lambda: z_far[r, h].start())
        pl.when(first_row)(lambda: y_up_far[r, h].start())
        pl.when(second_row)(lambda: y_down_near[r, h].start())

    def pass_far(r, h):
        z_far[r, h].wait_recv()
        pl.when(second_row)(lambda: y_down_far[r, h].start())

    pass_mate(0)
    pl.when(has_prev)(lambda: pass_near(0, 0))
    send_q.start()
    ask(x, store_own)
    total[...] = jnp.zeros_like(total)
    mass[...] = jnp.zeros_like(mass)
    pass_mate(1)
    pl.when(has_prev)(lambda: pass_near(0, 1))

    inner = 1.0 / (math.sqrt(HD) * softcap_limit)
    outer = softcap_limit / math.log(2.0)

    def attend(block, first, last, distances):
        keys_here = rows // PIECES

        def tile(t, carry):
            side = t // tiles_per_side
            within = t % tiles_per_side
            head = within // tiles_per_head
            start = pl.multiple_of((within % tiles_per_head) * ROW_TILE, ROW_TILE)
            q = queries[side, head, pl.ds(start, ROW_TILE), :]
            part = None
            added = None
            for h in range(PIECES):
                scores = lax.dot_general(
                    q, block[h, 0], (((1,), (1,)), ((), ())), preferred_element_type=jnp.float32
                )
                weights = jnp.exp2(outer * jnp.tanh(scores * inner))
                if distances is not None:
                    distance = jnp.where(side == 0, distances[0], distances[1])
                    offset = (
                        distance * rows
                        + start
                        - h * keys_here
                        + lax.broadcasted_iota(jnp.int32, weights.shape, 0)
                        - lax.broadcasted_iota(jnp.int32, weights.shape, 1)
                    )
                    weights = jnp.where((offset >= 0) & (offset < WINDOW), weights, 0.0)
                for k in range(keys_here // 128):
                    lanes = weights[:, k * 128 : (k + 1) * 128]
                    part = lanes if part is None else part + lanes
                product = jnp.dot(
                    weights.astype(jnp.bfloat16), block[h, 1], preferred_element_type=jnp.float32
                )
                added = product if added is None else added + product
            mass[side, head, pl.ds(start, ROW_TILE), :] += part
            total[side, head, pl.ds(start, ROW_TILE), :] += added
            return carry

        lax.fori_loop(first, last, tile, 0)

    both = 2 * tiles_per_side
    reach = WINDOW // rows

    def ahead(d, r, side):
        if side == r:
            return jnp.int32(2 * d)
        return 2 * d + (2 * x - 1 if side == 0 else 1 - 2 * x)

    def edge(d, r):
        return (ahead(d, r, 0), ahead(d, r, 1))

    def bounds(d, r):
        low, high = edge(d, r)
        fits = lambda e: (e >= 0) & (e <= reach)
        first = jnp.where(fits(low), 0, tiles_per_side)
        last = jnp.where(fits(high), both, tiles_per_side)
        return first, last

    def whole(slot, r):
        attend(held.at[slot, r], 0, both, None)

    def arrive_near(r):
        for h in range(PIECES):
            y_up_near[r, h].wait_recv()
        whole(1, r)

    def arrive_far(r):
        for h in range(PIECES):
            y_up_far[r, h].wait_recv()
        whole(3, r)

    def farthest(r):
        first, last = bounds(4, r)
        attend(held.at[4, r], first, last, edge(4, r))

    attend(kv_ref.at[x], 0, tiles_per_side, edge(0, 0))
    pl.when(has_prev)(lambda: pass_near(1, 0))
    send_q.wait_recv()
    pl.when(has_prev)(lambda: pass_near(1, 1))
    attend(kv_ref.at[x], tiles_per_side, bounds(0, 0)[1], edge(0, 0))
    first, last = bounds(0, 1)
    attend(held.at[0, 1], first, last, edge(0, 1))
    pl.when(has_far)(lambda: pass_far(0, 0))
    pl.when(has_prev)(lambda: whole(2, 0))
    pl.when(has_far)(lambda: pass_far(0, 1))
    pl.when(has_prev)(lambda: whole(2, 1))
    pl.when(me >= 2)(lambda: arrive_near(0))
    pl.when(has_far)(lambda: pass_far(1, 0))
    pl.when(has_far)(lambda: farthest(0))
    pl.when(has_far)(lambda: pass_far(1, 1))
    pl.when(me >= 2)(lambda: arrive_near(1))
    pl.when(has_far)(lambda: farthest(1))
    pl.when(me >= 6)(lambda: arrive_far(0))
    pl.when(me >= 6)(lambda: arrive_far(1))

    def finished(side, head):
        weight = jnp.sum(mass[side, head], axis=-1, keepdims=True)
        return (total[side, head] / weight).astype(jnp.bfloat16)

    send_out = [copy(X_OUT + head, leaving.at[head], landed.at[head], x_mate) for head in range(2)]
    leaving[0] = finished(1, 0)
    leaving[1] = finished(1, 1)
    send_out[0].start()
    for head in range(2):
        at = pl.multiple_of((2 * x + head) * HD, HD)
        out_ref[:, pl.ds(at, HD)] = finished(0, head)
        if head == 0:
            send_out[1].start()
    for head in range(2):
        send_out[head].wait_recv()
        at = pl.multiple_of((2 * (1 - x) + head) * HD, HD)
        out_ref[:, pl.ds(at, HD)] = landed[head]

    send_q.wait_send()
    for h in range(PIECES):
        send_kv[h].wait_send()
        send_out[h].wait_send()
    for r, h in pieces:
        pl.when(has_next)(lambda: z_near[r, h].wait_send())
        pl.when(has_next & has_prev)(lambda: z_far[r, h].wait_send())
        pl.when(first_row)(lambda: y_up_near[r, h].wait_send())
        pl.when(first_row & has_prev)(lambda: y_up_far[r, h].wait_send())
        pl.when(second_row & has_prev)(lambda: y_down_near[r, h].wait_send())
        pl.when(second_row & has_far)(lambda: y_down_far[r, h].wait_send())


def attention(normed, weight, cosine, sine, kv, blocks):
    rows = normed.shape[0]
    half = (2, rows, HD)
    vmem = pl.BlockSpec(memory_space=pltpu.VMEM)
    return pl.pallas_call(
        functools.partial(attention_kernel, blocks, rows),
        out_shape=jax.ShapeDtypeStruct((rows, 4 * HD), jnp.bfloat16),
        in_specs=[vmem] * 5,
        out_specs=vmem,
        scratch_shapes=[
            pltpu.VMEM((5, 2) + kv.shape[1:], jnp.bfloat16),
            pltpu.VMEM((2,) + half, jnp.bfloat16),
            pltpu.VMEM(half, jnp.bfloat16),
            pltpu.VMEM((2,) + half, jnp.float32),
            pltpu.VMEM((2, 2, rows, 128), jnp.float32),
            pltpu.VMEM(half, jnp.bfloat16),
            pltpu.VMEM(half, jnp.bfloat16),
            pltpu.SemaphoreType.DMA((MESSAGES,)),
            pltpu.SemaphoreType.DMA((MESSAGES,)),
        ],
        compiler_params=pltpu.CompilerParams(
            collective_id=0, has_side_effects=True, vmem_limit_bytes=48 * 1024 * 1024
        ),
    )(normed, weight, cosine, sine, kv)


def norm_kernel(own_ref, other_ref, gain_ref, out_ref):
    side = lax.axis_index("head")
    width = own_ref.shape[1]
    own = own_ref[...].astype(jnp.float32)
    other = other_ref[...].astype(jnp.float32)
    squares = jnp.sum(own * own, axis=-1, keepdims=True)
    squares = squares + jnp.sum(other * other, axis=-1, keepdims=True)
    scale = lax.rsqrt(squares / (2 * width) + norm_epsilon)
    for values, place in ((own, side), (other, 1 - side)):
        at = pl.ds(pl.multiple_of(place * width, width), width)
        out_ref[:, at] = (values * scale * gain_ref[:, at]).astype(jnp.bfloat16)


def norm(own, other, gain):
    rows, width = own.shape
    step = rows // 8
    return pl.pallas_call(
        norm_kernel,
        grid=(rows // step,),
        out_shape=jax.ShapeDtypeStruct((rows, 2 * width), jnp.bfloat16),
        in_specs=[
            pl.BlockSpec((step, width), lambda i: (i, 0)),
            pl.BlockSpec((step, width), lambda i: (i, 0)),
            pl.BlockSpec((1, 2 * width), lambda i: (0, 0)),
        ],
        out_specs=pl.BlockSpec((step, 2 * width), lambda i: (i, 0)),
    )(own, other, gain[None, :])


def swap_heads(shard):
    return lax.ppermute(shard, "head", [(0, 1), (1, 0)])


def rope_tables(positions):
    midpoint = HD // 2
    frequency = jnp.exp(
        -jnp.log(rope_base) * (2.0 * jnp.arange(midpoint, dtype=jnp.float32) / HD)
    )
    angles = positions.astype(jnp.float32)[:, None] * frequency[None, :]
    return jnp.cos(angles), jnp.sin(angles)


def rotated(head, cosine, sine):
    midpoint = HD // 2
    leading, trailing = head[:, :midpoint], head[:, midpoint:]
    return jnp.concatenate(
        [leading * cosine - trailing * sine, trailing * cosine + leading * sine], axis=-1
    ).astype(jnp.bfloat16)


def local(blocks, tokens, pre_gain, query_weight, key_weight, value_weight, out_weight, post_gain):
    rows, width = tokens.shape
    side = lax.axis_index("head")
    other = swap_heads(tokens)
    normed = norm(tokens, other, pre_gain)
    positions = lax.axis_index("seq") * rows + jnp.arange(rows, dtype=jnp.int32)
    cosine, sine = rope_tables(positions)
    project = lambda weight: jnp.dot(normed, weight, preferred_element_type=jnp.float32)
    k_all, v_all = project(key_weight), project(value_weight)
    head_of = lambda a, h: a[:, h * HD : (h + 1) * HD]
    in_pieces = lambda a: a.reshape(PIECES, rows // PIECES, HD)
    kv = jnp.stack(
        [
            jnp.stack(
                [
                    in_pieces(rotated(head_of(k_all, k), cosine, sine)),
                    in_pieces(head_of(v_all, k).astype(jnp.bfloat16)),
                ],
                axis=1,
            )
            for k in range(2)
        ]
    )
    attended = attention(normed, query_weight, cosine, sine, kv, blocks)
    mine = lax.dynamic_slice_in_dim(out_weight, side * width, width, 1)
    theirs = lax.dynamic_slice_in_dim(out_weight, (1 - side) * width, width, 1)
    given = jnp.dot(attended, theirs, preferred_element_type=jnp.float32).astype(jnp.bfloat16)
    arrived = swap_heads(given)
    kept = jnp.dot(attended, mine, preferred_element_type=jnp.float32)
    share = kept + arrived.astype(jnp.float32)
    squares = jnp.sum(share * share, axis=1, keepdims=True)
    squares = squares + swap_heads(squares)
    inverse_rms = lax.rsqrt(squares / (2 * width) + norm_epsilon)
    return (tokens.astype(jnp.float32) + post_gain * share * inverse_rms).astype(jnp.bfloat16)


def solution(mesh):
    placed = (
        P("seq", "head"),
        P(),
        P(None, "head"),
        P(None, "head"),
        P(None, "head"),
        P("head", None),
        P("head"),
    )
    return jax.shard_map(
        functools.partial(local, mesh.shape["seq"]),
        mesh=mesh,
        in_specs=placed,
        out_specs=P("seq", "head"),
        check_vma=False,
    )
```

```python
import functools
import math

import jax
import jax.numpy as jnp
from jax import lax
from jax.experimental import pallas as pl
from jax.experimental.pallas import tpu as pltpu
from jax.sharding import PartitionSpec as P

HD = 256
WINDOW = 4096

softcap_limit = 50.0
rope_base = 10000.0
norm_epsilon = 1e-06

ROW_TILE = 512

PIECES = 2
X_KV, X_Q, X_OUT, Z_NEAR, Z_FAR, Y_NEAR, Y_FAR, MESSAGES = 0, 2, 3, 5, 9, 13, 17, 21


def attention_kernel(
    blocks, rows, normed_ref, weight_ref, cosine_ref, sine_ref, kv_ref, out_ref,
    held, queries, asked, total, mass, leaving, landed, send_sems, recv_sems,
):
    group = 2 * 2
    me = lax.axis_index("seq")
    x = me % 2
    y = (me // 2) % 2
    x_mate = me + 1 - 2 * x
    y_mate = me + 2 - 4 * y
    z_next = me + group
    has_next = z_next < blocks
    has_prev = me >= group
    has_far = me >= 2 * group
    first_row = y == 0
    second_row = y == 1

    def copy(message, src, dst, device):
        return pltpu.make_async_remote_copy(
            src_ref=src,
            dst_ref=dst,
            send_sem=send_sems.at[message],
            recv_sem=recv_sems.at[message],
            device_id={"seq": device},
            device_id_type=pl.DeviceIdType.MESH,
        )

    barrier = pltpu.get_barrier_semaphore()

    def greet(device):
        pl.semaphore_signal(
            barrier, inc=1, device_id={"seq": device}, device_id_type=pl.DeviceIdType.MESH
        )

    greet(x_mate)
    greet(y_mate)
    pl.when(has_next)(lambda: greet(z_next))
    pl.when(has_prev)(lambda: greet(me - group))
    pl.semaphore_wait(barrier, 2 + has_next.astype(jnp.int32) + has_prev.astype(jnp.int32))

    pieces = [(r, h) for r in range(2) for h in range(PIECES)]
    near = lambda r, h: kv_ref.at[x, h] if r == 0 else held.at[0, 1, h]

    def copies(base, source, slot, device):
        return {
            (r, h): copy(base + PIECES * r + h, source(r, h), held.at[slot, r, h], device)
            for r, h in pieces
        }

    arrived = lambda slot: lambda r, h: held.at[slot, r, h]
    send_kv = [
        copy(X_KV + h, kv_ref.at[1 - x, h], held.at[0, 1, h], x_mate) for h in range(PIECES)
    ]
    send_q = copy(X_Q, asked, queries.at[1], x_mate)
    z_near = copies(Z_NEAR, near, 2, z_next)
    z_far = copies(Z_FAR, arrived(2), 4, z_next)
    y_up_near = copies(Y_NEAR, near, 1, y_mate)
    y_up_far = copies(Y_FAR, arrived(2), 3, y_mate)
    y_down_near = copies(Y_NEAR, arrived(2), 1, y_mate)
    y_down_far = copies(Y_FAR, arrived(4), 3, y_mate)

    for h in range(PIECES):
        send_kv[h].start()
        pl.when(has_next)(lambda: z_near[0, h].start())
        pl.when(first_row)(lambda: y_up_near[0, h].start())

    tiles_per_side = 2 * rows // ROW_TILE
    tiles_per_head = rows // ROW_TILE

    def ask(whose, store):
        def tile(t, carry):
            head = t // tiles_per_head
            start = pl.multiple_of((t % tiles_per_head) * ROW_TILE, ROW_TILE)
            at = pl.multiple_of((2 * whose + head) * HD, HD)
            value = jnp.dot(
                normed_ref[pl.ds(start, ROW_TILE), :],
                weight_ref[:, pl.ds(at, HD)],
                preferred_element_type=jnp.float32,
            )
            store(
                head,
                pl.ds(start, ROW_TILE),
                rotated(
                    value,
                    cosine_ref[pl.ds(start, ROW_TILE), :],
                    sine_ref[pl.ds(start, ROW_TILE), :],
                ),
            )
            return carry

        lax.fori_loop(0, tiles_per_side, tile, 0)

    def store_asked(head, where, value):
        asked[head, where, :] = value

    def store_own(head, where, value):
        queries[0, head, where, :] = value

    ask(1 - x, store_asked)

    def pass_mate(h):
        send_kv[h].wait_recv()
        pl.when(has_next)(lambda: z_near[1, h].start())
        pl.when(first_row)(lambda: y_up_near[1, h].start())

    def pass_near(r, h):
        z_near[r, h].wait_recv()
        pl.when(has_next)(lambda: z_far[r, h].start())
        pl.when(first_row)(lambda: y_up_far[r, h].start())
        pl.when(second_row)(lambda: y_down_near[r, h].start())

    def pass_far(r, h):
        z_far[r, h].wait_recv()
        pl.when(second_row)(lambda: y_down_far[r, h].start())

    pass_mate(0)
    pl.when(has_prev)(lambda: pass_near(0, 0))
    send_q.start()
    ask(x, store_own)
    total[...] = jnp.zeros_like(total)
    mass[...] = jnp.zeros_like(mass)
    pass_mate(1)
    pl.when(has_prev)(lambda: pass_near(0, 1))

    inner = 1.0 / (math.sqrt(HD) * softcap_limit)
    outer = softcap_limit / math.log(2.0)

    def attend(block, first, last, distances):
        keys_here = rows // PIECES

        def tile(t, carry):
            side = t // tiles_per_side
            within = t % tiles_per_side
            head = within // tiles_per_head
            start = pl.multiple_of((within % tiles_per_head) * ROW_TILE, ROW_TILE)
            q = queries[side, head, pl.ds(start, ROW_TILE), :]
            part = None
            added = None
            for h in range(PIECES):
                scores = lax.dot_general(
                    q, block[h, 0], (((1,), (1,)), ((), ())), preferred_element_type=jnp.float32
                )
                weights = jnp.exp2(outer * jnp.tanh(scores * inner))
                if distances is not None:
                    distance = jnp.where(side == 0, distances[0], distances[1])
                    offset = (
                        distance * rows
                        + start
                        - h * keys_here
                        + lax.broadcasted_iota(jnp.int32, weights.shape, 0)
                        - lax.broadcasted_iota(jnp.int32, weights.shape, 1)
                    )
                    weights = jnp.where((offset >= 0) & (offset < WINDOW), weights, 0.0)
                for k in range(keys_here // 128):
                    lanes = weights[:, k * 128 : (k + 1) * 128]
                    part = lanes if part is None else part + lanes
                product = jnp.dot(
                    weights.astype(jnp.bfloat16), block[h, 1], preferred_element_type=jnp.float32
                )
                added = product if added is None else added + product
            mass[side, head, pl.ds(start, ROW_TILE), :] += part
            total[side, head, pl.ds(start, ROW_TILE), :] += added
            return carry

        lax.fori_loop(first, last, tile, 0)

    both = 2 * tiles_per_side
    reach = WINDOW // rows

    def ahead(d, r, side):
        if side == r:
            return jnp.int32(2 * d)
        return 2 * d + (2 * x - 1 if side == 0 else 1 - 2 * x)

    def edge(d, r):
        return (ahead(d, r, 0), ahead(d, r, 1))

    def bounds(d, r):
        low, high = edge(d, r)
        fits = lambda e: (e >= 0) & (e <= reach)
        first = jnp.where(fits(low), 0, tiles_per_side)
        last = jnp.where(fits(high), both, tiles_per_side)
        return first, last

    def whole(slot, r):
        attend(held.at[slot, r], 0, both, None)

    def arrive_near(r):
        for h in range(PIECES):
            y_up_near[r, h].wait_recv()
        whole(1, r)

    def arrive_far(r):
        for h in range(PIECES):
            y_up_far[r, h].wait_recv()
        whole(3, r)

    def farthest(r):
        first, last = bounds(4, r)
        attend(held.at[4, r], first, last, edge(4, r))

    attend(kv_ref.at[x], 0, tiles_per_side, edge(0, 0))
    pl.when(has_prev)(lambda: pass_near(1, 0))
    send_q.wait_recv()
    pl.when(has_prev)(lambda: pass_near(1, 1))
    attend(kv_ref.at[x], tiles_per_side, bounds(0, 0)[1], edge(0, 0))
    first, last = bounds(0, 1)
    attend(held.at[0, 1], first, last, edge(0, 1))
    pl.when(has_far)(lambda: pass_far(0, 0))
    pl.when(has_prev)(lambda: whole(2, 0))
    pl.when(has_far)(lambda: pass_far(0, 1))
    pl.when(has_prev)(lambda: whole(2, 1))
    pl.when(me >= 2)(lambda: arrive_near(0))
    pl.when(has_far)(lambda: pass_far(1, 0))
    pl.when(has_far)(lambda: farthest(0))
    pl.when(has_far)(lambda: pass_far(1, 1))
    pl.when(me >= 2)(lambda: arrive_near(1))
    pl.when(has_far)(lambda: farthest(1))
    pl.when(me >= 6)(lambda: arrive_far(0))
    pl.when(me >= 6)(lambda: arrive_far(1))

    def finished(side, head):
        weight = jnp.sum(mass[side, head], axis=-1, keepdims=True)
        return (total[side, head] / weight).astype(jnp.bfloat16)

    send_out = [copy(X_OUT + head, leaving.at[head], landed.at[head], x_mate) for head in range(2)]
    leaving[0] = finished(1, 0)
    leaving[1] = finished(1, 1)
    send_out[0].start()
    for head in range(2):
        at = pl.multiple_of((2 * x + head) * HD, HD)
        out_ref[:, pl.ds(at, HD)] = finished(0, head)
        if head == 0:
            send_out[1].start()
    for head in range(2):
        send_out[head].wait_recv()
        at = pl.multiple_of((2 * (1 - x) + head) * HD, HD)
        out_ref[:, pl.ds(at, HD)] = landed[head]

    send_q.wait_send()
    for h in range(PIECES):
        send_kv[h].wait_send()
        send_out[h].wait_send()
    for r, h in pieces:
        pl.when(has_next)(lambda: z_near[r, h].wait_send())
        pl.when(has_next & has_prev)(lambda: z_far[r, h].wait_send())
        pl.when(first_row)(lambda: y_up_near[r, h].wait_send())
        pl.when(first_row & has_prev)(lambda: y_up_far[r, h].wait_send())
        pl.when(second_row & has_prev)(lambda: y_down_near[r, h].wait_send())
        pl.when(second_row & has_far)(lambda: y_down_far[r, h].wait_send())


def attention(normed, weight, cosine, sine, kv, blocks):
    rows = normed.shape[0]
    half = (2, rows, HD)
    vmem = pl.BlockSpec(memory_space=pltpu.VMEM)
    return pl.pallas_call(
        functools.partial(attention_kernel, blocks, rows),
        out_shape=jax.ShapeDtypeStruct((rows, 4 * HD), jnp.bfloat16),
        in_specs=[vmem] * 5,
        out_specs=vmem,
        scratch_shapes=[
            pltpu.VMEM((5, 2) + kv.shape[1:], jnp.bfloat16),
            pltpu.VMEM((2,) + half, jnp.bfloat16),
            pltpu.VMEM(half, jnp.bfloat16),
            pltpu.VMEM((2,) + half, jnp.float32),
            pltpu.VMEM((2, 2, rows, 128), jnp.float32),
            pltpu.VMEM(half, jnp.bfloat16),
            pltpu.VMEM(half, jnp.bfloat16),
            pltpu.SemaphoreType.DMA((MESSAGES,)),
            pltpu.SemaphoreType.DMA((MESSAGES,)),
        ],
        compiler_params=pltpu.CompilerParams(
            collective_id=0, has_side_effects=True, vmem_limit_bytes=48 * 1024 * 1024
        ),
    )(normed, weight, cosine, sine, kv)


def norm_kernel(own_ref, other_ref, gain_ref, out_ref):
    side = lax.axis_index("head")
    width = own_ref.shape[1]
    lines = 16

    def chunk(i, carry):
        at_rows = pl.ds(pl.multiple_of(i * lines, lines), lines)
        squares = jnp.zeros((lines, 1), jnp.float32)
        for ref in (own_ref, other_ref):
            values = ref[at_rows, :].astype(jnp.float32)
            squares = squares + jnp.sum(values * values, axis=-1, keepdims=True)
        scale = lax.rsqrt(squares / (2 * width) + norm_epsilon)
        for ref, place in ((own_ref, side), (other_ref, 1 - side)):
            at = pl.ds(pl.multiple_of(place * width, width), width)
            values = ref[at_rows, :].astype(jnp.float32)
            out_ref[at_rows, at] = (values * scale * gain_ref[:, at]).astype(jnp.bfloat16)
        return carry

    lax.fori_loop(0, own_ref.shape[0] // lines, chunk, 0, unroll=2)


def norm(own, other, gain):
    rows, width = own.shape
    step = rows // 4
    return pl.pallas_call(
        norm_kernel,
        grid=(rows // step,),
        out_shape=jax.ShapeDtypeStruct((rows, 2 * width), jnp.bfloat16),
        in_specs=[
            pl.BlockSpec((step, width), lambda i: (i, 0)),
            pl.BlockSpec((step, width), lambda i: (i, 0)),
            pl.BlockSpec((1, 2 * width), lambda i: (0, 0)),
        ],
        out_specs=pl.BlockSpec((step, 2 * width), lambda i: (i, 0)),
    )(own, other, gain[None, :])


def swap_heads(shard):
    return lax.ppermute(shard, "head", [(0, 1), (1, 0)])


def rope_tables(positions):
    midpoint = HD // 2
    frequency = jnp.exp(
        -jnp.log(rope_base) * (2.0 * jnp.arange(midpoint, dtype=jnp.float32) / HD)
    )
    angles = positions.astype(jnp.float32)[:, None] * frequency[None, :]
    return jnp.cos(angles), jnp.sin(angles)


def rotated(head, cosine, sine):
    midpoint = HD // 2
    leading, trailing = head[:, :midpoint], head[:, midpoint:]
    return jnp.concatenate(
        [leading * cosine - trailing * sine, trailing * cosine + leading * sine], axis=-1
    ).astype(jnp.bfloat16)


def local(blocks, tokens, pre_gain, query_weight, key_weight, value_weight, out_weight, post_gain):
    rows, width = tokens.shape
    side = lax.axis_index("head")
    other = swap_heads(tokens)
    normed = norm(tokens, other, pre_gain)
    positions = lax.axis_index("seq") * rows + jnp.arange(rows, dtype=jnp.int32)
    cosine, sine = rope_tables(positions)
    project = lambda weight: jnp.dot(normed, weight, preferred_element_type=jnp.float32)
    k_all, v_all = project(key_weight), project(value_weight)
    head_of = lambda a, h: a[:, h * HD : (h + 1) * HD]
    in_pieces = lambda a: a.reshape(PIECES, rows // PIECES, HD)
    kv = jnp.stack(
        [
            jnp.stack(
                [
                    in_pieces(rotated(head_of(k_all, k), cosine, sine)),
                    in_pieces(head_of(v_all, k).astype(jnp.bfloat16)),
                ],
                axis=1,
            )
            for k in range(2)
        ]
    )
    attended = attention(normed, query_weight, cosine, sine, kv, blocks)
    mine = lax.dynamic_slice_in_dim(out_weight, side * width, width, 1)
    theirs = lax.dynamic_slice_in_dim(out_weight, (1 - side) * width, width, 1)
    given = jnp.dot(attended, theirs, preferred_element_type=jnp.float32).astype(jnp.bfloat16)
    arrived = swap_heads(given)
    kept = jnp.dot(attended, mine, preferred_element_type=jnp.float32)
    share = kept + arrived.astype(jnp.float32)
    squares = jnp.sum(share * share, axis=1, keepdims=True)
    squares = squares + swap_heads(squares)
    inverse_rms = lax.rsqrt(squares / (2 * width) + norm_epsilon)
    return (tokens.astype(jnp.float32) + post_gain * share * inverse_rms).astype(jnp.bfloat16)


def solution(mesh):
    placed = (
        P("seq", "head"),
        P(),
        P(None, "head"),
        P(None, "head"),
        P(None, "head"),
        P("head", None),
        P("head"),
    )
    return jax.shard_map(
        functools.partial(local, mesh.shape["seq"]),
        mesh=mesh,
        in_specs=placed,
        out_specs=P("seq", "head"),
        check_vma=False,
    )
```
